32 devices in a mesh: dp: 8 (over z, x), mp: 4 (over y, core).
Axes of the slice: x: 2, y: 2, z: 4, core: 2. Of those that a mesh axis runs over, the one named last changes fastest.
Arguments:
- tokens: bfloat16 [1024, 4096], P('dp'), may hold values from -6 to 6
- cotangent: bfloat16 [1024, 4096], P('dp', 'mp'), may hold values from -6 to 6
- sketch: float32 [4096, 128], P('dp'), may hold values from -12 to 12
Outputs:
- precond: bfloat16 [4096, 4096], P('dp', 'mp')
- new_sketch: float32 [4096, 128], P('dp')
The draws below stay inside these ranges and needn't reach their ends.
All inputs are finite; a program needn't handle non-finite values.
Results may differ from the reference program's by a relative error of at most 0.001.
Values sent between devices are 32-bit elements; how exact they have to be, the bound alone decides.
A program may use at most 64 MiB of HBM per device.

```python
import math
import jax
import jax.numpy as jnp
from jax import lax

D = 4096
COLS = 4096
RANK = 128
ITERS = 1
TOKENS = 1024


def strengthened(entries, stream_key, source, target, blocks, factor):
    owner, partner = [(jnp.arange(entries.shape[position]) // (entries.shape[position] // blocks)).reshape([-1 if axis == position else 1 for axis in range(entries.ndim)]) for position in (source, target)]
    chosen = jax.random.permutation(stream_key, blocks)[partner]
    strong = (owner == chosen) | (owner == (partner + blocks // 2) % blocks)
    return jnp.where(strong, factor * entries, entries)


def shard_levels(stream_key, dims, pieces, least, top_value):
    factor_of = 1.0
    for dim, shards_of in pieces:
        steps = jax.random.uniform(jax.random.fold_in(jax.random.fold_in(stream_key, 6), dim), (shards_of,), jnp.float32, least / len(pieces), top_value / len(pieces))
        factor_of = factor_of * jnp.repeat(jnp.exp(steps), dims[dim] // shards_of).reshape((-1,) + (1,) * (len(dims) - 1 - dim))
    return factor_of


def gaussian(rng, dims, deviation, most, pieces=(), kind=jnp.bfloat16):
    factor_of = shard_levels(rng, dims, pieces, -0.22, 0.18) if pieces else 1.0
    array = jax.random.normal(rng, dims, jnp.float32) * deviation * factor_of
    return jnp.minimum(jnp.maximum(array, -most), most).astype(kind)


def bell_draw_with(stream_key, dims, scale, bound, pieces, heavy, held_as=jnp.bfloat16):
    entries = scale * jax.random.normal(stream_key, dims, jnp.float32)
    if pieces:
        entries = entries * shard_levels(stream_key, dims, pieces, -0.22, 0.18)
    return jnp.clip(strengthened(entries, jax.random.fold_in(stream_key, 3), *heavy), -bound, bound).astype(held_as)


def setup_inputs(seed: int = 0) -> dict:
    streams_of = jax.random.split(jax.random.key(seed), 4)
    return {
        "tokens": bell_draw_with(streams_of[0], (TOKENS, D), 1.0, 6.0, ((0, 8),), (0, 1, 8, 2.0)),
        "cotangent": gaussian(streams_of[1], (TOKENS, COLS), 1.0, 6.0, ((0, 8), (1, 4))),
        "sketch": gaussian(streams_of[2], (D, RANK), 2.0, 12.0, ((0, 8),), jnp.float32),
    }


DECAY_RATE = 0.9
RIDGE_FRAC = 0.0001

def product(left_mat, right_mat):
    return jnp.dot(left_mat, right_mat, precision=lax.Precision.HIGHEST)

def right_solve(values, lower_tri):
    return lax.linalg.triangular_solve(lower_tri, values, left_side=False, lower=True, transpose_a=True)

def left_solve(lower_tri, values, transpose):
    return lax.linalg.triangular_solve(lower_tri, values, left_side=True, lower=True, transpose_a=transpose)

def spd_solve(matrix, target):
    lower_tri = jnp.linalg.cholesky(matrix)
    return left_solve(lower_tri, left_solve(lower_tri, target, False), True)

def reference(tokens, cotangent, sketch):
    gradient = jnp.dot(tokens.T.astype(jnp.float32), cotangent.astype(jnp.float32), preferred_element_type=jnp.float32) * (1.0 / math.sqrt(TOKENS))

    def covariance(basis_now):
        return DECAY_RATE * product(sketch, product(sketch.T, basis_now)) + product(gradient, product(gradient.T, basis_now))
    basis_now = sketch
    for iteration in range(ITERS):
        applied = covariance(basis_now)
        basis_now = right_solve(applied, jnp.linalg.cholesky(product(applied.T, applied)))
    applied = covariance(basis_now)
    rayleigh = product(basis_now.T, applied)
    rayleigh = 0.5 * (rayleigh + rayleigh.T)
    mean_level = jnp.trace(rayleigh) / RANK
    identity = jnp.eye(RANK, dtype=jnp.float32)
    new_sketch = right_solve(applied, jnp.linalg.cholesky(rayleigh + RIDGE_FRAC * mean_level * identity))
    inner_mat = mean_level * identity + product(new_sketch.T, new_sketch)
    coeffs = spd_solve(inner_mat, product(new_sketch.T, gradient))
    precond = gradient - product(new_sketch, coeffs)
    return (precond.astype(jnp.bfloat16), new_sketch)
```

```python
import functools
import math

import jax
import jax.numpy as jnp
from jax import lax
from jax.experimental import pallas as pl
from jax.experimental.pallas import tpu as pltpu
from jax.sharding import PartitionSpec as P

DECAY_RATE = 0.9
RIDGE_FRAC = 0.0001
MESH = pl.DeviceIdType.MESH
VMEM = pltpu.MemorySpace.VMEM
VMEM_BUDGET = 48 * 2**20


def product(left_mat, right_mat, dims=((1,), (0,))):
    return lax.dot_general(
        left_mat,
        right_mat,
        (dims, ((), ())),
        precision=lax.Precision.HIGHEST,
        preferred_element_type=jnp.float32,
    )


TN = ((0,), (0,))
NT = ((1,), (1,))


def remote(src, dst, send, recv, where):
    return pltpu.make_async_remote_copy(
        src_ref=src,
        dst_ref=dst,
        send_sem=send,
        recv_sem=recv,
        device_id=where,
        device_id_type=MESH,
    )


def inverse_factor(matrix):
    n = matrix.shape[0]
    start = jnp.where(
        lax.broadcasted_iota(jnp.int32, (n, n), 0) == lax.broadcasted_iota(jnp.int32, (n, n), 1), 1.0, 0.0
    ).astype(jnp.float32)
    left = [matrix[8 * i : 8 * i + 8] for i in range(n // 8)]
    right = [start[8 * i : 8 * i + 8] for i in range(n // 8)]
    row_of = lax.broadcasted_iota(jnp.int32, (8, 1), 0)
    rows = []
    for j in range(0, n, 2):
        t, s = divmod(j, 8)
        a0, a1 = left[t][s : s + 1], left[t][s + 1 : s + 2]
        b0, b1 = right[t][s : s + 1], right[t][s + 1 : s + 2]
        pivot, side, corner = a0[:, j : j + 1], a0[:, j + 1 : j + 2], a1[:, j + 1 : j + 2]
        inv0 = 1.0 / pivot
        factor = side * inv0
        a1, b1 = a1 - factor * a0, b1 - factor * b0
        second = corner - factor * side
        inv1 = 1.0 / second
        rows += [b0 * lax.rsqrt(pivot), b1 * lax.rsqrt(second)]
        a0, b0, a1, b1 = a0 * inv0, b0 * inv0, a1 * inv1, b1 * inv1
        for i in range(t, n // 8):
            c0, c1 = left[i][:, j : j + 1], left[i][:, j + 1 : j + 2]
            c1 = c1 - factor * c0
            if i == t:
                c0 = jnp.where(row_of > s + 1, c0, 0.0)
                c1 = jnp.where(row_of > s + 1, c1, 0.0)
            left[i] = left[i] - c0 * a0 - c1 * a1
            right[i] = right[i] - c0 * b0 - c1 * b1
    return jnp.concatenate(rows, axis=0)


def factor_kernel(matrix_ref, inverse_ref):
    inverse_ref[...] = inverse_factor(matrix_ref[...])


def finish_kernel(low_ref, cross_ref, self_ref, new_ref, mixer_ref):
    rank_size = low_ref.shape[0]
    half = product(low_ref[...], cross_ref[...])
    rayleigh = 0.5 * (half + half.T)
    square = (rank_size, rank_size)
    diagonal = lax.broadcasted_iota(jnp.int32, square, 0) == lax.broadcasted_iota(jnp.int32, square, 1)
    mean_level = jnp.sum(jnp.where(diagonal, rayleigh, 0.0)) / rank_size
    shifted = rayleigh + jnp.where(diagonal, RIDGE_FRAC * mean_level, 0.0)
    new_inv = inverse_factor(shifted)
    new_ref[...] = new_inv
    self_gram = product(product(new_inv, self_ref[...]), new_inv, NT)
    inner_inv = inverse_factor(self_gram + jnp.where(diagonal, mean_level, 0.0))
    mixer_ref[...] = product(inner_inv.T, product(inner_inv, new_inv))


def small_call(kernel, count, name, *arrays):
    shape = jax.ShapeDtypeStruct(arrays[0].shape, jnp.float32)
    return pl.pallas_call(
        kernel,
        out_shape=(shape,) * count,
        in_specs=[pl.BlockSpec(memory_space=VMEM)] * len(arrays),
        out_specs=(pl.BlockSpec(memory_space=VMEM),) * count,
        name=name,
    )(*arrays)


def reduce_kernel(axis, n, with_factor, *refs):
    if with_factor:
        x_ref, matrix_ref, o_ref, inverse_ref, *refs = refs
    else:
        x_ref, o_ref, *refs = refs
    land, own, send_a, recv_a, send_b, recv_b = refs
    me = lax.axis_index(axis)
    chunk = own.shape[0]
    barrier = pltpu.get_barrier_semaphore()
    peers = [lax.rem(me + k, n) for k in range(1, n)]
    for peer in peers:
        pl.semaphore_signal(barrier, inc=1, device_id={axis: peer}, device_id_type=MESH)
    pl.semaphore_wait(barrier, n - 1)
    scatter = [
        remote(
            x_ref.at[pl.ds(pl.multiple_of(peer * chunk, 8), chunk)],
            land.at[k],
            send_a.at[k],
            recv_a.at[k],
            {axis: peer},
        )
        for k, peer in enumerate(peers)
    ]
    for copy in scatter:
        copy.start()
    if with_factor:
        inverse_ref[...] = inverse_factor(matrix_ref[...])
    mine = pl.ds(pl.multiple_of(me * chunk, 8), chunk)
    total = x_ref[mine]
    for k, copy in enumerate(scatter):
        copy.wait_recv()
        total = total + land[k]
    own[...] = total
    gather = [
        remote(own, o_ref.at[mine], send_b.at[k], recv_b.at[k], {axis: peer})
        for k, peer in enumerate(peers)
    ]
    for copy in gather:
        copy.start()
    o_ref[mine] = total
    for copy in scatter:
        copy.wait_send()
    for copy in gather:
        copy.wait()


def all_sum(arrays, axis, ident, matrix=None):
    n = lax.axis_size(axis)
    rows = sum(a.shape[0] for a in arrays)
    if rows % (8 * n) or n > 16:
        summed = lax.psum(tuple(arrays), axis)
        return summed if matrix is None else summed + small_call(factor_kernel, 1, "factor", matrix)
    joined = arrays[0] if len(arrays) == 1 else jnp.concatenate(arrays, axis=0)
    width = joined.shape[1]
    chunk = rows // n
    operands = (joined,) if matrix is None else (joined, matrix)
    summed, *inverse = pl.pallas_call(
        functools.partial(reduce_kernel, axis, n, matrix is not None),
        out_shape=tuple(jax.ShapeDtypeStruct(a.shape, jnp.float32) for a in operands),
        in_specs=[pl.BlockSpec(memory_space=VMEM)] * len(operands),
        out_specs=(pl.BlockSpec(memory_space=VMEM),) * len(operands),
        scratch_shapes=[
            pltpu.VMEM((n - 1, chunk, width), jnp.float32),
            pltpu.VMEM((chunk, width), jnp.float32),
        ]
        + [pltpu.SemaphoreType.DMA((n - 1,))] * 4,
        compiler_params=pltpu.CompilerParams(collective_id=ident, has_side_effects=True),
        name=f"sum_{axis}_{ident}",
    )(*operands)
    outs, at = [], 0
    for a in arrays:
        outs.append(summed[at : at + a.shape[0]])
        at += a.shape[0]
    return tuple(outs + inverse)


def gradient_kernel(
    nd, nm, pieces, scale, x_ref, y_ref, g_ref, xland, yland, xt, yb,
    local, xs, xr, ms, mr, zs, zr, fs, fr, os, orr,
):
    d, m = lax.axis_index("dp"), lax.axis_index("mp")
    rows, block = xland.shape[1], xland.shape[2]
    share = rows // nm
    nz = nd // 2
    z, x = lax.div(d, 2), lax.rem(d, 2)
    other = 2 * z + 1 - x
    barrier = pltpu.get_barrier_semaphore()
    for k in range(1, nd):
        pl.semaphore_signal(barrier, inc=1, device_id={"dp": lax.rem(d + k, nd)}, device_id_type=MESH)
    for k in range(1, nm):
        pl.semaphore_signal(barrier, inc=1, device_id={"mp": lax.rem(m + k, nm)}, device_id_type=MESH)
    pl.semaphore_wait(barrier, nd + nm - 2)

    part = pl.ds(pl.multiple_of(m * share, 8), share)
    x_out = []
    for k in range(1, nd):
        peer = lax.rem(d + k, nd)
        cols = pl.ds(pl.multiple_of(peer * block, 128), block)
        x_out.append(
            remote(x_ref.at[part, cols], xland.at[d, part], xs.at[k - 1], xr.at[k - 1], {"dp": peer})
        )
    piece = rows // pieces
    cuts = [pl.ds(c * piece, piece) for c in range(pieces)]

    def along(way, k, c):
        source = 2 * (z - way * k) + x
        at = yland.at[source, cuts[c]]
        return remote(
            y_ref.at[cuts[c]] if k == 0 else at,
            at,
            zs.at[(way + 1) // 2, k, c],
            zr.at[(way + 1) // 2, k, c],
            {"dp": 2 * (z + way) + x},
        )

    def across(way, k, c):
        at = yland.at[2 * (z - way * (k + 1)) + x, cuts[c]]
        return remote(at, at, fs.at[(way + 1) // 2, k, c], fr.at[(way + 1) // 2, k, c], {"dp": other})

    def inside(place):
        return jnp.logical_and(place >= 0, place < nz)

    def sends(way, k):
        return jnp.logical_and(inside(z - way * k), inside(z + way))

    def streams(steps):
        return [(way, k, c) for k in range(steps) for c in range(pieces) for way in (1, -1)]

    over = [
        remote(y_ref.at[cut], yland.at[d, cut], os.at[c], orr.at[c], {"dp": other})
        for c, cut in enumerate(cuts)
    ]
    for c in range(pieces):
        for way in (1, -1):
            pl.when(sends(way, 0))(lambda way=way, c=c: along(way, 0, c).start())
        over[c].start()
        if c == 0:
            for copy in x_out:
                copy.start()
    mine = pl.ds(pl.multiple_of(d * block, 128), block)
    keep_x = pltpu.make_async_copy(x_ref.at[:, mine], xland.at[d], local.at[0])
    keep_y = pltpu.make_async_copy(y_ref, yland.at[d], local.at[1])
    keep_x.start()
    keep_y.start()

    passed = []
    for k in range(1, nd):
        x_out[k - 1].wait_recv()
        source = lax.rem(d + nd - k, nd)
        for j in range(1, nm):
            copy = remote(
                xland.at[source, part],
                xland.at[source, part],
                ms.at[k - 1, j - 1],
                mr.at[k - 1, j - 1],
                {"mp": lax.rem(m + j, nm)},
            )
            copy.start()
            passed.append(copy)
    for way, k, c in streams(nz - 1):

        @pl.when(inside(z - way * (k + 1)))
        def _():
            along(way, k, c).wait_recv()
            across(way, k, c).start()

            if k + 1 < nz - 1:

                @pl.when(inside(z + way))
                def _():
                    along(way, k + 1, c).start()

    keep_x.wait()
    keep_y.wait()
    for copy in passed:
        copy.wait_recv()
    for s in range(nd):
        xt[:, s * rows : (s + 1) * rows] = xland[s].T.astype(jnp.bfloat16)
    for copy in over:
        copy.wait_recv()
    for way, k, c in streams(nz - 1):
        pl.when(inside(z - way * (k + 1)))(lambda way=way, k=k, c=c: across(way, k, c).wait())
    for s in range(nd):
        yb[s * rows : (s + 1) * rows, :] = yland[s].astype(jnp.bfloat16)
    width = yb.shape[1]
    tile = 256 if width % 256 == 0 else width

    def body(t, carry):
        cols = pl.ds(pl.multiple_of(t * tile, 128), tile)
        g_ref[:, cols] = scale * jnp.dot(xt[...], yb[:, cols], preferred_element_type=jnp.float32)
        return carry

    lax.fori_loop(0, width // tile, body, 0)
    for copy in x_out + passed + over:
        copy.wait_send()
    for way, k, c in streams(nz - 1):
        pl.when(sends(way, k))(lambda way=way, k=k, c=c: along(way, k, c).wait_send())


def gradient_block(tokens, cotangent, norm_scale):
    nd, nm = lax.axis_size("dp"), lax.axis_size("mp")
    rows, depth = tokens.shape
    width = cotangent.shape[1]
    block = depth // nd
    need = 4 * rows * (depth + width) + 6 * nd * rows * (block + width) + 4 * block * width
    if need > VMEM_BUDGET or nd % 2 or rows % (8 * nm) or block % 128 or width % 128:
        partial = lax.dot_general(
            tokens, cotangent, (((0,), (0,)), ((), ())), preferred_element_type=jnp.float32
        )
        return lax.psum_scatter(partial * norm_scale, "dp", scatter_dimension=0, tiled=True)
    nz = nd // 2
    pieces = 2 if rows % 16 == 0 else 1
    dma = pltpu.SemaphoreType.DMA
    return pl.pallas_call(
        functools.partial(gradient_kernel, nd, nm, pieces, norm_scale),
        out_shape=jax.ShapeDtypeStruct((block, width), jnp.float32),
        in_specs=[pl.BlockSpec(memory_space=VMEM)] * 2,
        out_specs=pl.BlockSpec(memory_space=VMEM),
        scratch_shapes=[
            pltpu.VMEM((nd, rows, block), jnp.float32),
            pltpu.VMEM((nd, rows, width), jnp.float32),
            pltpu.VMEM((block, nd * rows), jnp.bfloat16),
            pltpu.VMEM((nd * rows, width), jnp.bfloat16),
            dma((2,)),
            dma((nd - 1,)),
            dma((nd - 1,)),
            dma((nd - 1, nm - 1)),
            dma((nd - 1, nm - 1)),
            dma((2, nz - 1, pieces)),
            dma((2, nz - 1, pieces)),
            dma((2, nz - 1, pieces)),
            dma((2, nz - 1, pieces)),
            dma((pieces,)),
            dma((pieces,)),
        ],
        compiler_params=pltpu.CompilerParams(
            collective_id=0, has_side_effects=True, vmem_limit_bytes=60 * 2**20
        ),
        name="gradient_block",
    )(tokens.astype(jnp.float32), cotangent.astype(jnp.float32))


def halves(value, axis):
    high = value.astype(jnp.bfloat16)
    low = (value - high.astype(jnp.float32)).astype(jnp.bfloat16)
    return jnp.concatenate([high, low], axis=axis)


def folded(value, axis):
    n = value.shape[axis] // 2
    if axis == 0:
        return value[:n] + value[n:]
    return value[:, :n] + value[:, n:]


def exact_left(left, right):
    return folded(jnp.dot(left, halves(right, 1), preferred_element_type=jnp.float32), 1)


def exact_right(left, right):
    return folded(jnp.dot(halves(left, 0), right, preferred_element_type=jnp.float32), 0)


def times(left, right):
    both = halves(right, 1)
    full = jnp.concatenate([both, both], axis=0)
    return folded(jnp.dot(halves(left, 1), full, preferred_element_type=jnp.float32), 1)


def gram(left, right):
    full = jnp.dot(halves(left.T, 0), halves(right, 1), preferred_element_type=jnp.float32)
    return folded(folded(full, 0), 1)


def factor_steps(matrix, result):
    n = matrix.shape[0]
    start = jnp.where(
        lax.broadcasted_iota(jnp.int32, (n, n), 0) == lax.broadcasted_iota(jnp.int32, (n, n), 1), 1.0, 0.0
    ).astype(jnp.float32)
    left = [matrix[8 * i : 8 * i + 8] for i in range(n // 8)]
    right = [start[8 * i : 8 * i + 8] for i in range(n // 8)]
    row_of = lax.broadcasted_iota(jnp.int32, (8, 1), 0)
    rows = []
    for j in range(0, n, 2):
        t, s = divmod(j, 8)
        a0, a1 = left[t][s : s + 1], left[t][s + 1 : s + 2]
        b0, b1 = right[t][s : s + 1], right[t][s + 1 : s + 2]
        pivot, side, corner = a0[:, j : j + 1], a0[:, j + 1 : j + 2], a1[:, j + 1 : j + 2]
        inv0 = 1.0 / pivot
        factor = side * inv0
        a1, b1 = a1 - factor * a0, b1 - factor * b0
        second = corner - factor * side
        inv1 = 1.0 / second
        rows += [b0 * lax.rsqrt(pivot), b1 * lax.rsqrt(second)]
        a0, b0, a1, b1 = a0 * inv0, b0 * inv0, a1 * inv1, b1 * inv1
        for i in range(t, n // 8):
            c0, c1 = left[i][:, j : j + 1], left[i][:, j + 1 : j + 2]
            c1 = c1 - factor * c0
            if i == t:
                c0 = jnp.where(row_of > s + 1, c0, 0.0)
                c1 = jnp.where(row_of > s + 1, c1, 0.0)
            left[i] = left[i] - c0 * a0 - c1 * a1
            right[i] = right[i] - c0 * b0 - c1 * b1
        if s == 6:
            yield
    result.append(jnp.concatenate(rows, axis=0))


def run_with(steps, actions):
    actions = list(actions)
    for _ in steps:
        if actions:
            actions.pop(0)()
    for action in actions:
        action()


def whole_kernel(nd, nm, pieces, scale, tok_ref, cot_ref, s_ref, pre_ref, new_ref, *refs):
    (
        xf, yf, xland, yland, xt, xb, yb, g, upart, uland, uown, u, kept, ssf,
        ppart, pland, psum, pother, w,
        local, xs, xr, ms, mr, zs, zr, fs, fr, os, orr,
        us, ur, gs, gr, ss, sr, ys, yr, cs, cr, ks, kr,
        ps, pr, qs, qr, ts, tr,
    ) = refs
    d, m = lax.axis_index("dp"), lax.axis_index("mp")
    rows, block = xland.shape[1], xland.shape[2]
    width = yb.shape[1]
    rank = s_ref.shape[1]
    share = rows // nm
    count = nd * rows
    quarter = count // nm
    slab = rank // nd
    nz = nd // 2
    z, x = lax.div(d, 2), lax.rem(d, 2)
    other = 2 * z + 1 - x
    my, mc = lax.div(m, 2), lax.rem(m, 2)
    mate = 2 * my + 1 - mc
    facing = 2 * (1 - my) + mc
    barrier = pltpu.get_barrier_semaphore()
    for k in range(1, nd):
        pl.semaphore_signal(barrier, inc=1, device_id={"dp": lax.rem(d + k, nd)}, device_id_type=MESH)
    for k in range(1, nm):
        pl.semaphore_signal(barrier, inc=1, device_id={"mp": lax.rem(m + k, nm)}, device_id_type=MESH)
    yf[...] = cot_ref[...].astype(jnp.float32)
    xf[...] = tok_ref[...].astype(jnp.float32)
    pl.semaphore_wait(barrier, nd + nm - 2)

    part = pl.ds(pl.multiple_of(m * share, 8), share)
    x_out = []
    for k in range(1, nd):
        peer = lax.rem(d + k, nd)
        cols = pl.ds(pl.multiple_of(peer * block, 128), block)
        x_out.append(remote(xf.at[part, cols], xland.at[d, part], xs.at[k - 1], xr.at[k - 1], {"dp": peer}))
    piece = rows // pieces
    cuts = [pl.ds(c * piece, piece) for c in range(pieces)]

    def along(way, k, c):
        source = 2 * (z - way * k) + x
        at = yland.at[source, cuts[c]]
        return remote(
            yf.at[cuts[c]] if k == 0 else at,
            at,
            zs.at[(way + 1) // 2, k, c],
            zr.at[(way + 1) // 2, k, c],
            {"dp": 2 * (z + way) + x},
        )

    def across(way, k, c):
        at = yland.at[2 * (z - way * (k + 1)) + x, cuts[c]]
        return remote(at, at, fs.at[(way + 1) // 2, k, c], fr.at[(way + 1) // 2, k, c], {"dp": other})

    def inside(place):
        return jnp.logical_and(place >= 0, place < nz)

    def sends(way, k):
        return jnp.logical_and(inside(z - way * k), inside(z + way))

    def streams(steps):
        return [(way, k, c) for k in range(steps) for c in range(pieces) for way in (1, -1)]

    over = [
        remote(yf.at[cut], yland.at[d, cut], os.at[c], orr.at[c], {"dp": other}) for c, cut in enumerate(cuts)
    ]
    for c in range(pieces):
        for way in (1, -1):
            pl.when(sends(way, 0))(lambda way=way, c=c: along(way, 0, c).start())
        over[c].start()
        if c == 0:
            for copy in x_out:
                copy.start()
    mine = pl.ds(pl.multiple_of(d * block, 128), block)
    keep_x = pltpu.make_async_copy(xf.at[:, mine], xland.at[d], local.at[0])
    keep_y = pltpu.make_async_copy(yf, yland.at[d], local.at[1])
    keep_x.start()
    keep_y.start()

    passed = []
    for k in range(1, nd):
        x_out[k - 1].wait_recv()
        source = lax.rem(d + nd - k, nd)
        for j in range(1, nm):
            copy = remote(
                xland.at[source, part],
                xland.at[source, part],
                ms.at[k - 1, j - 1],
                mr.at[k - 1, j - 1],
                {"mp": lax.rem(m + j, nm)},
            )
            copy.start()
            passed.append(copy)

    def place(mm, dd):
        return pl.ds(pl.multiple_of((mm * nd + dd) * share, 8), share)

    pending = list(x_out) + passed + over

    def behind(k):
        return lax.rem(d + nd - k, nd)

    def reduce(a, k):
        peer = lax.rem(d + k, nd)
        size = share + slab if a == 0 else share
        return remote(
            upart.at[a, peer, pl.ds(0, size)], uland.at[a, d, pl.ds(0, size)],
            us.at[a, k - 1], ur.at[a, k - 1], {"dp": peer},
        )

    def gather(a, k):
        return remote(
            uown.at[a, pl.ds(0, share)], u.at[a, place(m, d)],
            gs.at[a, k - 1], gr.at[a, k - 1], {"dp": lax.rem(d + k, nd)},
        )

    def gather_slab(k):
        return remote(
            uown.at[0, pl.ds(share, slab)], ssf.at[pl.ds(pl.multiple_of(d * slab, 8), slab)],
            ss.at[k - 1], sr.at[k - 1], {"dp": lax.rem(d + k, nd)},
        )

    def hop(a, k, owner, send, recv, to):
        at = u.at[a, place(owner, behind(k))]
        source = uown.at[a, pl.ds(0, share)] if k == 0 and send is not ks else at
        return remote(source, at, send.at[a, k], recv.at[a, k], {"mp": to})

    def to_facing(a, k):
        return hop(a, k, m, ys, yr, facing)

    def to_mate(a, k):
        return hop(a, k, m, cs, cr, mate)

    def on_to_mate(a, k):
        return hop(a, k, facing, ks, kr, mate)

    def sum_start(a, value, extra=None):
        some = exact_left(xb[pl.ds(pl.multiple_of(m * quarter, 8), quarter), :], value)
        upart[a, :, :share] = some.reshape(nd, share, rank)
        if extra is not None:
            upart[a, :, share:] = extra.reshape(nd, slab, rank)
        for k in range(1, nd):
            reduce(a, k).start()

    def sum_own(a):
        size = share + slab if a == 0 else share
        total = upart[a, d, :size]
        for k in range(1, nd):
            reduce(a, k).wait_recv()
            total = total + uland[a, behind(k), :size]
        uown[a, :size] = total
        for k in range(1, nd):
            gather(a, k).start()
        to_facing(a, 0).start()
        to_mate(a, 0).start()
        if a == 0:
            for k in range(1, nd):
                gather_slab(k).start()
            ssf[pl.ds(pl.multiple_of(d * slab, 8), slab)] = total[share:]
        u[a, place(m, d)] = total[:share]

    def sum_pass(a, ks_):
        for k in ks_:
            gather(a, k).wait_recv()
            to_facing(a, k).start()
            to_mate(a, k).start()

    def sum_cross(a, ks_):
        for k in ks_:
            hop(a, k, facing, ys, yr, facing).wait_recv()
            on_to_mate(a, k).start()

    def sum_end(a):
        for k in range(nd):
            to_mate(a, k).wait_recv()
            on_to_mate(a, k).wait_recv()
        if a == 0:
            for k in range(1, nd):
                gather_slab(k).wait_recv()

    def sum_drain(a):
        for k in range(1, nd):
            reduce(a, k).wait_send()
            gather(a, k).wait_send()
            if a == 0:
                gather_slab(k).wait_send()
        for k in range(nd):
            to_facing(a, k).wait_send()
            to_mate(a, k).wait_send()
            on_to_mate(a, k).wait_send()

    bands, half = w.shape[1], w.shape[3]

    def to_core(a, q):
        return remote(ppart.at[a, q, 1 - mc], pland.at[a, q], ps.at[a, q], pr.at[a, q], {"mp": mate})

    def to_chip(a, q):
        return remote(psum.at[a, q], pother.at[a, q], qs.at[a, q], qr.at[a, q], {"mp": facing})

    def back(a, q):
        at = w.at[a, q, mc]
        return remote(at, at, ts.at[a, q], tr.at[a, q], {"mp": mate})

    def images(a, value):
        span = exact_right(value.T, yb[...]).T
        both = halves(span, 1)
        for q in range(bands):
            some = jnp.dot(yb[q * 2 * half : (q + 1) * 2 * half, :], both, preferred_element_type=jnp.float32)
            ppart[a, q] = (folded(some, 1) * (scale * scale)).reshape(2, half, rank)
            to_core(a, q).start()

    def image_chip(a, q):
        to_core(a, q).wait_recv()
        psum[a, q] = ppart[a, q, mc] + pland[a, q]
        to_chip(a, q).start()

    def image_sum(a, q):
        to_chip(a, q).wait_recv()
        w[a, q, mc] = psum[a, q] + pother[a, q]
        back(a, q).start()

    def image_end(a):
        for q in range(bands):
            back(a, q).wait_recv()
        return w[a].reshape(count, rank)

    def image_drain(a):
        for q in range(bands):
            to_core(a, q).wait_send()
            to_chip(a, q).wait_send()
            back(a, q).wait_send()

    def first_sum():
        keep_x.wait()
        for copy in passed:
            copy.wait_recv()
        for s in range(nd):
            xt[:, s * rows : (s + 1) * rows] = xland[s].T.astype(jnp.bfloat16)
            xb[s * rows : (s + 1) * rows, :] = xland[s].astype(jnp.bfloat16)
        sketch = s_ref[...]
        sum_start(0, sketch, gram(sketch, sketch))

    def relay(steps):
        for way, k, c in steps:

            @pl.when(inside(z - way * (k + 1)))
            def _():
                along(way, k, c).wait_recv()
                across(way, k, c).start()

                if k + 1 < nz - 1:

                    @pl.when(inside(z + way))
                    def _():
                        along(way, k + 1, c).start()

    waves = streams(nz - 1)
    per = 2 * pieces
    relay(waves[:per])
    first_sum()
    relay(waves[per : 2 * per])
    sum_own(0)
    relay(waves[2 * per :])
    sum_pass(0, range(1, nd))
    sum_cross(0, range(nd))
    sum_end(0)
    keep_y.wait()
    for copy in over:
        copy.wait_recv()
    for way, k, c in waves:
        pl.when(inside(z - way * (k + 1)))(lambda way=way, k=k, c=c: across(way, k, c).wait())
    for s in range(nd):
        yb[s * rows : (s + 1) * rows, :] = yland[s].astype(jnp.bfloat16)

    square = (rank, rank)
    diagonal = lax.broadcasted_iota(jnp.int32, square, 0) == lax.broadcasted_iota(jnp.int32, square, 1)
    tile = 256 if width % 256 == 0 else width

    def gradient_tile(t, carry):
        cols = pl.ds(pl.multiple_of(t * tile, 128), tile)
        g[:, cols] = scale * jnp.dot(xt[...], yb[:, cols], preferred_element_type=jnp.float32)
        return carry

    images(0, u[0])
    for q in range(bands):
        image_chip(0, q)
    sketch_gram = ssf[...]
    lax.fori_loop(0, width // tile, gradient_tile, 0)
    for q in range(bands):
        image_sum(0, q)
    w0 = image_end(0)
    sum_start(1, exact_left(xt[...], w0))
    mixed0 = DECAY_RATE * times(u[0], sketch_gram)
    proj1 = DECAY_RATE * times(sketch_gram, sketch_gram) + gram(u[0], w0)
    sum_own(1)
    sum_pass(1, range(1, nd))
    sum_cross(1, range(nd))
    sum_end(1)
    kept[...] = mixed0 + u[1]
    images(1, kept[...])
    gram_mat = DECAY_RATE * times(sketch_gram, proj1) + gram(w0, kept[...])
    low = []
    run_with(
        factor_steps(gram_mat, low),
        [functools.partial(image_chip, 1, q) for q in range(bands)]
        + [lambda: None] * 2
        + [functools.partial(image_sum, 1, q) for q in range(bands)],
    )
    low_t = low[0].T
    w1 = times(image_end(1), low_t)
    moved = exact_left(xt[...], w1)
    sum_start(2, moved)
    u1 = times(kept[...], low_t)
    proj1 = times(proj1, low_t)
    rayleigh = DECAY_RATE * gram(proj1, proj1) + gram(u1, w1)
    rayleigh = 0.5 * (rayleigh + rayleigh.T)
    mean_level = jnp.sum(jnp.where(diagonal, rayleigh, 0.0)) / rank
    shifted = rayleigh + jnp.where(diagonal, RIDGE_FRAC * mean_level, 0.0)
    applied = DECAY_RATE * times(s_ref[...], proj1) + moved
    proj2 = DECAY_RATE * times(sketch_gram, proj1) + gram(u[0], w1)
    mixed1 = DECAY_RATE * times(u[0], proj1)
    self_part = DECAY_RATE * gram(proj1, proj2) + mean_level * shifted
    top = []
    run_with(
        factor_steps(shifted, top),
        [lambda: sum_own(2)]
        + [functools.partial(sum_pass, 2, [k]) for k in range(1, nd)]
        + [functools.partial(sum_cross, 2, [k]) for k in range(nd)],
    )
    new_ref[...] = times(applied, top[0].T)
    sum_end(2)
    u2 = mixed1 + u[2]
    bottom = []
    run_with(factor_steps(self_part + gram(w1, u2), bottom), [])
    span = scale * exact_right(u2.T, yb[...])
    mixer = halves(times(times(applied, bottom[0].T), bottom[0]), 1)
    both = halves(span, 0)
    high = jnp.concatenate([both[:rank], both[:rank]], axis=0)
    low = jnp.concatenate([both[rank:], both[rank:]], axis=0)
    for t in range(width // tile):
        cols = slice(t * tile, (t + 1) * tile)
        gone = jnp.dot(mixer, high[:, cols], preferred_element_type=jnp.float32)
        gone = gone + jnp.dot(mixer, low[:, cols], preferred_element_type=jnp.float32)
        pre_ref[:, cols] = (g[:, cols] - gone).astype(jnp.bfloat16)

    for copy in pending:
        copy.wait_send()
    for way, k, c in waves:
        pl.when(sends(way, k))(lambda way=way, k=k, c=c: along(way, k, c).wait_send())
    for a in range(3):
        sum_drain(a)
    for a in range(2):
        image_drain(a)


def whole_fits(tokens, cotangent, sketch):
    nd, nm = lax.axis_size("dp"), lax.axis_size("mp")
    rows, depth = tokens.shape
    width = cotangent.shape[1]
    block, rank = sketch.shape
    need = 4 * rows * (depth + width) + nd * rows * (8 * block + 6 * width) + 4 * block * width
    need += 54 * nd * rows * rank
    return (
        nm == 4
        and nd % 2 == 0
        and nd <= 16
        and rank == 128
        and rows % 128 == 0
        and block % 128 == 0
        and width % 128 == 0
        and rank % (8 * nd) == 0
        and need <= VMEM_BUDGET
    )


def whole(tokens, cotangent, sketch, norm_scale):
    nd, nm = lax.axis_size("dp"), lax.axis_size("mp")
    rows, depth = tokens.shape
    width = cotangent.shape[1]
    block, rank = sketch.shape
    nz = nd // 2
    pieces = 2
    share, slab, count = rows // nm, rank // nd, nd * rows
    bands = 4
    half = count // (2 * bands)
    dma = pltpu.SemaphoreType.DMA
    f32 = jnp.float32
    return pl.pallas_call(
        functools.partial(whole_kernel, nd, nm, pieces, norm_scale),
        out_shape=(
            jax.ShapeDtypeStruct((block, width), jnp.bfloat16),
            jax.ShapeDtypeStruct((block, rank), f32),
        ),
        in_specs=[pl.BlockSpec(memory_space=VMEM)] * 3,
        out_specs=(pl.BlockSpec(memory_space=VMEM),) * 2,
        scratch_shapes=[
            pltpu.VMEM((rows, depth), f32),
            pltpu.VMEM((rows, width), f32),
            pltpu.VMEM((nd, rows, block), f32),
            pltpu.VMEM((nd, rows, width), f32),
            pltpu.VMEM((block, count), jnp.bfloat16),
            pltpu.VMEM((count, block), jnp.bfloat16),
            pltpu.VMEM((count, width), jnp.bfloat16),
            pltpu.VMEM((block, width), f32),
            pltpu.VMEM((3, nd, share + slab, rank), f32),
            pltpu.VMEM((3, nd, share + slab, rank), f32),
            pltpu.VMEM((3, share + slab, rank), f32),
            pltpu.VMEM((3, count, rank), f32),
            pltpu.VMEM((count, rank), f32),
            pltpu.VMEM((rank, rank), f32),
            pltpu.VMEM((2, bands, 2, half, rank), f32),
            pltpu.VMEM((2, bands, half, rank), f32),
            pltpu.VMEM((2, bands, half, rank), f32),
            pltpu.VMEM((2, bands, half, rank), f32),
            pltpu.VMEM((2, bands, 2, half, rank), f32),
            dma((2,)),
            dma((nd - 1,)),
            dma((nd - 1,)),
            dma((nd - 1, nm - 1)),
            dma((nd - 1, nm - 1)),
            dma((2, nz - 1, pieces)),
            dma((2, nz - 1, pieces)),
            dma((2, nz - 1, pieces)),
            dma((2, nz - 1, pieces)),
            dma((pieces,)),
            dma((pieces,)),
        ]
        + [dma((3, nd - 1))] * 4
        + [dma((nd - 1,))] * 2
        + [dma((3, nd))] * 6
        + [dma((2, bands))] * 6,
        compiler_params=pltpu.CompilerParams(
            collective_id=6, has_side_effects=True, vmem_limit_bytes=60 * 2**20
        ),
        name="whole",
    )(tokens, cotangent, sketch)


def shards(tokens, cotangent, sketch):
    norm_scale = 1.0 / math.sqrt(tokens.shape[0] * lax.axis_size("dp"))
    if whole_fits(tokens, cotangent, sketch):
        return whole(tokens, cotangent, sketch, norm_scale)
    gradient = gradient_block(tokens, cotangent, norm_scale)

    grad_proj, sketch_proj = all_sum(
        (product(gradient, sketch, TN), product(sketch, sketch, TN)), "dp", 1
    )
    (summed,) = all_sum((product(gradient, grad_proj),), "mp", 2)
    previous = DECAY_RATE * product(sketch, sketch_proj) + summed
    grad_image, sketch_image, gram_mat = all_sum(
        (
            product(gradient, previous, TN),
            product(sketch, previous, TN),
            product(previous, previous, TN),
        ),
        "dp",
        3,
    )
    summed, low_inv = all_sum((product(gradient, grad_image),), "mp", 4, gram_mat)
    applied = product(DECAY_RATE * product(sketch, sketch_image) + summed, low_inv, NT)
    image_grad, cross_prev, self_image = all_sum(
        (
            product(gradient, applied, TN),
            product(previous, applied, TN),
            product(applied, applied, TN),
        ),
        "dp",
        5,
    )
    new_inv, mixer = small_call(finish_kernel, 2, "finish", low_inv, cross_prev, self_image)
    new_sketch = product(applied, new_inv, NT)
    precond = gradient - product(product(new_sketch, mixer), image_grad, NT)
    return (precond.astype(jnp.bfloat16), new_sketch)


def solution(mesh):
    in_specs = (P("dp", None), P("dp", "mp"), P("dp", None))
    out_specs = (P("dp", "mp"), P("dp", None))
    return jax.shard_map(shards, mesh=mesh, in_specs=in_specs, out_specs=out_specs, check_vma=False)
```

```python
import functools
import math

import jax
import jax.numpy as jnp
from jax import lax
from jax.experimental import pallas as pl
from jax.experimental.pallas import tpu as pltpu
from jax.sharding import PartitionSpec as P

DECAY_RATE = 0.9
RIDGE_FRAC = 0.0001
MESH = pl.DeviceIdType.MESH
VMEM = pltpu.MemorySpace.VMEM
VMEM_BUDGET = 48 * 2**20


def product(left_mat, right_mat, dims=((1,), (0,))):
    return lax.dot_general(
        left_mat,
        right_mat,
        (dims, ((), ())),
        precision=lax.Precision.HIGHEST,
        preferred_element_type=jnp.float32,
    )


TN = ((0,), (0,))
NT = ((1,), (1,))


def remote(src, dst, send, recv, where):
    return pltpu.make_async_remote_copy(
        src_ref=src,
        dst_ref=dst,
        send_sem=send,
        recv_sem=recv,
        device_id=where,
        device_id_type=MESH,
    )


def inverse_factor(matrix):
    n = matrix.shape[0]
    start = jnp.where(
        lax.broadcasted_iota(jnp.int32, (n, n), 0) == lax.broadcasted_iota(jnp.int32, (n, n), 1), 1.0, 0.0
    ).astype(jnp.float32)
    left = [matrix[8 * i : 8 * i + 8] for i in range(n // 8)]
    right = [start[8 * i : 8 * i + 8] for i in range(n // 8)]
    row_of = lax.broadcasted_iota(jnp.int32, (8, 1), 0)
    rows = []
    for j in range(0, n, 2):
        t, s = divmod(j, 8)
        a0, a1 = left[t][s : s + 1], left[t][s + 1 : s + 2]
        b0, b1 = right[t][s : s + 1], right[t][s + 1 : s + 2]
        pivot, side, corner = a0[:, j : j + 1], a0[:, j + 1 : j + 2], a1[:, j + 1 : j + 2]
        inv0 = 1.0 / pivot
        factor = side * inv0
        a1, b1 = a1 - factor * a0, b1 - factor * b0
        second = corner - factor * side
        inv1 = 1.0 / second
        rows += [b0 * lax.rsqrt(pivot), b1 * lax.rsqrt(second)]
        a0, b0, a1, b1 = a0 * inv0, b0 * inv0, a1 * inv1, b1 * inv1
        for i in range(t, n // 8):
            c0, c1 = left[i][:, j : j + 1], left[i][:, j + 1 : j + 2]
            c1 = c1 - factor * c0
            if i == t:
                c0 = jnp.where(row_of > s + 1, c0, 0.0)
                c1 = jnp.where(row_of > s + 1, c1, 0.0)
            left[i] = left[i] - c0 * a0 - c1 * a1
            right[i] = right[i] - c0 * b0 - c1 * b1
    return jnp.concatenate(rows, axis=0)


def factor_kernel(matrix_ref, inverse_ref):
    inverse_ref[...] = inverse_factor(matrix_ref[...])


def finish_kernel(low_ref, cross_ref, self_ref, new_ref, mixer_ref):
    rank_size = low_ref.shape[0]
    half = product(low_ref[...], cross_ref[...])
    rayleigh = 0.5 * (half + half.T)
    square = (rank_size, rank_size)
    diagonal = lax.broadcasted_iota(jnp.int32, square, 0) == lax.broadcasted_iota(jnp.int32, square, 1)
    mean_level = jnp.sum(jnp.where(diagonal, rayleigh, 0.0)) / rank_size
    shifted = rayleigh + jnp.where(diagonal, RIDGE_FRAC * mean_level, 0.0)
    new_inv = inverse_factor(shifted)
    new_ref[...] = new_inv
    self_gram = product(product(new_inv, self_ref[...]), new_inv, NT)
    inner_inv = inverse_factor(self_gram + jnp.where(diagonal, mean_level, 0.0))
    mixer_ref[...] = product(inner_inv.T, product(inner_inv, new_inv))


def small_call(kernel, count, name, *arrays):
    shape = jax.ShapeDtypeStruct(arrays[0].shape, jnp.float32)
    return pl.pallas_call(
        kernel,
        out_shape=(shape,) * count,
        in_specs=[pl.BlockSpec(memory_space=VMEM)] * len(arrays),
        out_specs=(pl.BlockSpec(memory_space=VMEM),) * count,
        name=name,
    )(*arrays)


def reduce_kernel(axis, n, with_factor, *refs):
    if with_factor:
        x_ref, matrix_ref, o_ref, inverse_ref, *refs = refs
    else:
        x_ref, o_ref, *refs = refs
    land, own, send_a, recv_a, send_b, recv_b = refs
    me = lax.axis_index(axis)
    chunk = own.shape[0]
    barrier = pltpu.get_barrier_semaphore()
    peers = [lax.rem(me + k, n) for k in range(1, n)]
    for peer in peers:
        pl.semaphore_signal(barrier, inc=1, device_id={axis: peer}, device_id_type=MESH)
    pl.semaphore_wait(barrier, n - 1)
    scatter = [
        remote(
            x_ref.at[pl.ds(pl.multiple_of(peer * chunk, 8), chunk)],
            land.at[k],
            send_a.at[k],
            recv_a.at[k],
            {axis: peer},
        )
        for k, peer in enumerate(peers)
    ]
    for copy in scatter:
        copy.start()
    if with_factor:
        inverse_ref[...] = inverse_factor(matrix_ref[...])
    mine = pl.ds(pl.multiple_of(me * chunk, 8), chunk)
    total = x_ref[mine]
    for k, copy in enumerate(scatter):
        copy.wait_recv()
        total = total + land[k]
    own[...] = total
    gather = [
        remote(own, o_ref.at[mine], send_b.at[k], recv_b.at[k], {axis: peer})
        for k, peer in enumerate(peers)
    ]
    for copy in gather:
        copy.start()
    o_ref[mine] = total
    for copy in scatter:
        copy.wait_send()
    for copy in gather:
        copy.wait()


def all_sum(arrays, axis, ident, matrix=None):
    n = lax.axis_size(axis)
    rows = sum(a.shape[0] for a in arrays)
    if rows % (8 * n) or n > 16:
        summed = lax.psum(tuple(arrays), axis)
        return summed if matrix is None else summed + small_call(factor_kernel, 1, "factor", matrix)
    joined = arrays[0] if len(arrays) == 1 else jnp.concatenate(arrays, axis=0)
    width = joined.shape[1]
    chunk = rows // n
    operands = (joined,) if matrix is None else (joined, matrix)
    summed, *inverse = pl.pallas_call(
        functools.partial(reduce_kernel, axis, n, matrix is not None),
        out_shape=tuple(jax.ShapeDtypeStruct(a.shape, jnp.float32) for a in operands),
        in_specs=[pl.BlockSpec(memory_space=VMEM)] * len(operands),
        out_specs=(pl.BlockSpec(memory_space=VMEM),) * len(operands),
        scratch_shapes=[
            pltpu.VMEM((n - 1, chunk, width), jnp.float32),
            pltpu.VMEM((chunk, width), jnp.float32),
        ]
        + [pltpu.SemaphoreType.DMA((n - 1,))] * 4,
        compiler_params=pltpu.CompilerParams(collective_id=ident, has_side_effects=True),
        name=f"sum_{axis}_{ident}",
    )(*operands)
    outs, at = [], 0
    for a in arrays:
        outs.append(summed[at : at + a.shape[0]])
        at += a.shape[0]
    return tuple(outs + inverse)


def gradient_kernel(
    nd, nm, pieces, scale, x_ref, y_ref, g_ref, xland, yland, xt, yb,
    local, xs, xr, ms, mr, zs, zr, fs, fr, os, orr,
):
    d, m = lax.axis_index("dp"), lax.axis_index("mp")
    rows, block = xland.shape[1], xland.shape[2]
    share = rows // nm
    nz = nd // 2
    z, x = lax.div(d, 2), lax.rem(d, 2)
    other = 2 * z + 1 - x
    barrier = pltpu.get_barrier_semaphore()
    for k in range(1, nd):
        pl.semaphore_signal(barrier, inc=1, device_id={"dp": lax.rem(d + k, nd)}, device_id_type=MESH)
    for k in range(1, nm):
        pl.semaphore_signal(barrier, inc=1, device_id={"mp": lax.rem(m + k, nm)}, device_id_type=MESH)
    pl.semaphore_wait(barrier, nd + nm - 2)

    part = pl.ds(pl.multiple_of(m * share, 8), share)
    x_out = []
    for k in range(1, nd):
        peer = lax.rem(d + k, nd)
        cols = pl.ds(pl.multiple_of(peer * block, 128), block)
        x_out.append(
            remote(x_ref.at[part, cols], xland.at[d, part], xs.at[k - 1], xr.at[k - 1], {"dp": peer})
        )
    piece = rows // pieces
    cuts = [pl.ds(c * piece, piece) for c in range(pieces)]

    def along(way, k, c):
        source = 2 * (z - way * k) + x
        at = yland.at[source, cuts[c]]
        return remote(
            y_ref.at[cuts[c]] if k == 0 else at,
            at,
            zs.at[(way + 1) // 2, k, c],
            zr.at[(way + 1) // 2, k, c],
            {"dp": 2 * (z + way) + x},
        )

    def across(way, k, c):
        at = yland.at[2 * (z - way * (k + 1)) + x, cuts[c]]
        return remote(at, at, fs.at[(way + 1) // 2, k, c], fr.at[(way + 1) // 2, k, c], {"dp": other})

    def inside(place):
        return jnp.logical_and(place >= 0, place < nz)

    def sends(way, k):
        return jnp.logical_and(inside(z - way * k), inside(z + way))

    def streams(steps):
        return [(way, k, c) for k in range(steps) for c in range(pieces) for way in (1, -1)]

    over = [
        remote(y_ref.at[cut], yland.at[d, cut], os.at[c], orr.at[c], {"dp": other})
        for c, cut in enumerate(cuts)
    ]
    for c in range(pieces):
        for way in (1, -1):
            pl.when(sends(way, 0))(lambda way=way, c=c: along(way, 0, c).start())
        over[c].start()
        if c == 0:
            for copy in x_out:
                copy.start()
    mine = pl.ds(pl.multiple_of(d * block, 128), block)
    keep_x = pltpu.make_async_copy(x_ref.at[:, mine], xland.at[d], local.at[0])
    keep_y = pltpu.make_async_copy(y_ref, yland.at[d], local.at[1])
    keep_x.start()
    keep_y.start()

    passed = []
    for k in range(1, nd):
        x_out[k - 1].wait_recv()
        source = lax.rem(d + nd - k, nd)
        for j in range(1, nm):
            copy = remote(
                xland.at[source, part],
                xland.at[source, part],
                ms.at[k - 1, j - 1],
                mr.at[k - 1, j - 1],
                {"mp": lax.rem(m + j, nm)},
            )
            copy.start()
            passed.append(copy)
    for way, k, c in streams(nz - 1):

        @pl.when(inside(z - way * (k + 1)))
        def _():
            along(way, k, c).wait_recv()
            across(way, k, c).start()

            if k + 1 < nz - 1:

                @pl.when(inside(z + way))
                def _():
                    along(way, k + 1, c).start()

    keep_x.wait()
    keep_y.wait()
    for copy in passed:
        copy.wait_recv()
    for s in range(nd):
        xt[:, s * rows : (s + 1) * rows] = xland[s].T.astype(jnp.bfloat16)
    for copy in over:
        copy.wait_recv()
    for way, k, c in streams(nz - 1):
        pl.when(inside(z - way * (k + 1)))(lambda way=way, k=k, c=c: across(way, k, c).wait())
    for s in range(nd):
        yb[s * rows : (s + 1) * rows, :] = yland[s].astype(jnp.bfloat16)
    width = yb.shape[1]
    tile = 256 if width % 256 == 0 else width

    def body(t, carry):
        cols = pl.ds(pl.multiple_of(t * tile, 128), tile)
        g_ref[:, cols] = scale * jnp.dot(xt[...], yb[:, cols], preferred_element_type=jnp.float32)
        return carry

    lax.fori_loop(0, width // tile, body, 0)
    for copy in x_out + passed + over:
        copy.wait_send()
    for way, k, c in streams(nz - 1):
        pl.when(sends(way, k))(lambda way=way, k=k, c=c: along(way, k, c).wait_send())


def gradient_block(tokens, cotangent, norm_scale):
    nd, nm = lax.axis_size("dp"), lax.axis_size("mp")
    rows, depth = tokens.shape
    width = cotangent.shape[1]
    block = depth // nd
    need = 4 * rows * (depth + width) + 6 * nd * rows * (block + width) + 4 * block * width
    if need > VMEM_BUDGET or nd % 2 or rows % (8 * nm) or block % 128 or width % 128:
        partial = lax.dot_general(
            tokens, cotangent, (((0,), (0,)), ((), ())), preferred_element_type=jnp.float32
        )
        return lax.psum_scatter(partial * norm_scale, "dp", scatter_dimension=0, tiled=True)
    nz = nd // 2
    pieces = 2 if rows % 16 == 0 else 1
    dma = pltpu.SemaphoreType.DMA
    return pl.pallas_call(
        functools.partial(gradient_kernel, nd, nm, pieces, norm_scale),
        out_shape=jax.ShapeDtypeStruct((block, width), jnp.float32),
        in_specs=[pl.BlockSpec(memory_space=VMEM)] * 2,
        out_specs=pl.BlockSpec(memory_space=VMEM),
        scratch_shapes=[
            pltpu.VMEM((nd, rows, block), jnp.float32),
            pltpu.VMEM((nd, rows, width), jnp.float32),
            pltpu.VMEM((block, nd * rows), jnp.bfloat16),
            pltpu.VMEM((nd * rows, width), jnp.bfloat16),
            dma((2,)),
            dma((nd - 1,)),
            dma((nd - 1,)),
            dma((nd - 1, nm - 1)),
            dma((nd - 1, nm - 1)),
            dma((2, nz - 1, pieces)),
            dma((2, nz - 1, pieces)),
            dma((2, nz - 1, pieces)),
            dma((2, nz - 1, pieces)),
            dma((pieces,)),
            dma((pieces,)),
        ],
        compiler_params=pltpu.CompilerParams(
            collective_id=0, has_side_effects=True, vmem_limit_bytes=60 * 2**20
        ),
        name="gradient_block",
    )(tokens.astype(jnp.float32), cotangent.astype(jnp.float32))


def halves(value, axis):
    high = value.astype(jnp.bfloat16)
    low = (value - high.astype(jnp.float32)).astype(jnp.bfloat16)
    return jnp.concatenate([high, low], axis=axis)


def folded(value, axis):
    n = value.shape[axis] // 2
    if axis == 0:
        return value[:n] + value[n:]
    return value[:, :n] + value[:, n:]


def exact_left(left, right):
    return folded(jnp.dot(left, halves(right, 1), preferred_element_type=jnp.float32), 1)


def exact_right(left, right):
    return folded(jnp.dot(halves(left, 0), right, preferred_element_type=jnp.float32), 0)


def times(left, right):
    both = halves(right, 1)
    full = jnp.concatenate([both, both], axis=0)
    return folded(jnp.dot(halves(left, 1), full, preferred_element_type=jnp.float32), 1)


def gram(left, right):
    full = jnp.dot(halves(left.T, 0), halves(right, 1), preferred_element_type=jnp.float32)
    return folded(folded(full, 0), 1)


def spread(value, column):
    return jnp.take_along_axis(value, jnp.full(value.shape, column, jnp.int32), axis=1)


def factor_steps(matrix, result):
    n = matrix.shape[0]
    tile = (8, n)
    start = jnp.where(
        lax.broadcasted_iota(jnp.int32, (n, n), 0) == lax.broadcasted_iota(jnp.int32, (n, n), 1), 1.0, 0.0
    ).astype(jnp.float32)
    left = [matrix[8 * i : 8 * i + 8] for i in range(n // 8)]
    right = [start[8 * i : 8 * i + 8] for i in range(n // 8)]
    row_of = lax.broadcasted_iota(jnp.int32, tile, 0)
    rows = []

    def row(value, k):
        return jnp.broadcast_to(value[k : k + 1], tile)

    for t in range(n // 8):
        above, inverse = left[t], right[t]
        columns = [spread(above, 8 * t + k) for k in range(8)]
        done = []
        for k in range(8):
            pivot = row(columns[k], k)
            scale = 1.0 / pivot
            a, b = row(above, k) * scale, row(inverse, k) * scale
            rows.append((row(inverse, k) * lax.rsqrt(pivot))[:1])
            weights = [row(columns[q], k) * scale for q in range(k + 1, 8)]
            done.append((a, b, weights))
            c = jnp.where(row_of > k, columns[k], 0.0)
            above, inverse = above - c * a, inverse - c * b
            for q in range(k + 1, 8):
                columns[q] = columns[q] - c * weights[q - k - 1]
        for i in range(t + 1, n // 8):
            columns = [spread(left[i], 8 * t + k) for k in range(8)]
            for k, (a, b, weights) in enumerate(done):
                c = columns[k]
                left[i], right[i] = left[i] - c * a, right[i] - c * b
                for q in range(k + 1, 8):
                    columns[q] = columns[q] - c * weights[q - k - 1]
        yield
    result.append(jnp.concatenate(rows, axis=0))


def run_with(steps, actions):
    actions = list(actions)
    for _ in steps:
        if actions:
            actions.pop(0)()
    for action in actions:
        action()


def whole_kernel(nd, nm, pieces, scale, tok_ref, cot_ref, sketch_ref, g, mixer_ref, span_ref, new_ref, *refs):
    (
        tok, cot, s_ref, got, xf, yf, xland, yland, xt, xb, yb, upart, uland, uown, u, kept, ssf, wpart, wland, wsum,
        ppart, pland, psum, pother, w,
        local, xs, xr, ms, mr, zs, zr, fs, fr, os, orr,
        twins, twinr, us, ur, gs, gr, ss, sr, vs, vr, hs, hr, ys, yr, cs, cr, ks, kr,
        ps, pr, qs, qr, ts, tr,
    ) = refs
    d, m = lax.axis_index("dp"), lax.axis_index("mp")
    rows, block = xland.shape[1], xland.shape[2]
    width = yb.shape[1]
    rank = s_ref.shape[1]
    share = rows // nm
    count = nd * rows
    quarter = count // nm
    slab = rank // nd
    nz = nd // 2
    z, x = lax.div(d, 2), lax.rem(d, 2)
    other = 2 * z + 1 - x
    my, mc = lax.div(m, 2), lax.rem(m, 2)
    mate = 2 * my + 1 - mc
    facing = 2 * (1 - my) + mc
    barrier = pltpu.get_barrier_semaphore()
    for k in range(1, nd):
        pl.semaphore_signal(barrier, inc=1, device_id={"dp": lax.rem(d + k, nd)}, device_id_type=MESH)
    for k in range(1, nm):
        pl.semaphore_signal(barrier, inc=1, device_id={"mp": lax.rem(m + k, nm)}, device_id_type=MESH)
    fetch = [
        pltpu.make_async_copy(source, to, got.at[n])
        for n, (source, to) in enumerate([(tok_ref, tok), (cot_ref, cot), (sketch_ref, s_ref)])
    ]
    for copy in fetch:
        copy.start()
    for copy in fetch:
        copy.wait()
    xf[...] = tok[...].astype(jnp.float32)
    yf[...] = cot[...].astype(jnp.float32)
    pl.semaphore_wait(barrier, nd + nm - 2)

    part = pl.ds(pl.multiple_of(m * share, 8), share)
    x_out = []
    for k in range(1, nd):
        peer = lax.rem(d + k, nd)
        cols = pl.ds(pl.multiple_of(peer * block, 128), block)
        x_out.append(remote(xf.at[part, cols], xland.at[d, part], xs.at[k - 1], xr.at[k - 1], {"dp": peer}))
    piece = rows // pieces
    cuts = [pl.ds(c * piece, piece) for c in range(pieces)]

    def along(way, k, c):
        source = 2 * (z - way * k) + x
        at = yland.at[source, cuts[c]]
        return remote(
            yf.at[cuts[c]] if k == 0 else at,
            at,
            zs.at[(way + 1) // 2, k, c],
            zr.at[(way + 1) // 2, k, c],
            {"dp": 2 * (z + way) + x},
        )

    def across(way, k, c):
        at = yland.at[2 * (z - way * (k + 1)) + x, cuts[c]]
        return remote(at, at, fs.at[(way + 1) // 2, k, c], fr.at[(way + 1) // 2, k, c], {"dp": other})

    def inside(place):
        return jnp.logical_and(place >= 0, place < nz)

    def sends(way, k):
        return jnp.logical_and(inside(z - way * k), inside(z + way))

    def streams(steps):
        return [(way, k, c) for k in range(steps) for c in range(pieces) for way in (1, -1)]

    over = [
        remote(yf.at[cut], yland.at[d, cut], os.at[c], orr.at[c], {"dp": other}) for c, cut in enumerate(cuts)
    ]
    for copy in x_out:
        copy.start()
    for c in range(pieces):
        for way in (1, -1):
            pl.when(sends(way, 0))(lambda way=way, c=c: along(way, 0, c).start())
        over[c].start()
    mine = pl.ds(pl.multiple_of(d * block, 128), block)
    keep_x = pltpu.make_async_copy(xf.at[:, mine], xland.at[d], local.at[0])
    keep_y = pltpu.make_async_copy(yf, yland.at[d], local.at[1])
    keep_x.start()
    keep_y.start()

    def share_of(k, owner, way, to):
        at = xland.at[lax.rem(d + nd - k, nd), pl.ds(pl.multiple_of(owner * share, 8), share)]
        return remote(at, at, ms.at[k - 1, way], mr.at[k - 1, way], {"mp": to})

    passed = []
    for k in range(1, nd):
        x_out[k - 1].wait_recv()
        for way, to in ((0, facing), (1, mate)):
            copy = share_of(k, m, way, to)
            copy.start()
            passed.append(copy)

    def place(mm, dd):
        return pl.ds(pl.multiple_of((mm * nd + dd) * share, 8), share)

    pending = list(x_out) + passed + over

    def pass_on():
        for k in range(1, nd):
            share_of(k, facing, 0, facing).wait_recv()
            copy = share_of(k, facing, 2, mate)
            copy.start()
            pending.append(copy)

    def behind(k):
        return lax.rem(d + nd - k, nd)

    def reduce(a, k):
        peer = lax.rem(d + k, nd)
        size = share + slab if a == 0 else share
        return remote(
            upart.at[a, peer, pl.ds(0, size)], uland.at[a, d, pl.ds(0, size)],
            us.at[a, k - 1], ur.at[a, k - 1], {"dp": peer},
        )

    def gather(a, k):
        return remote(
            uown.at[a, pl.ds(0, share)], u.at[a, place(m, d)],
            gs.at[a, k - 1], gr.at[a, k - 1], {"dp": lax.rem(d + k, nd)},
        )

    def gather_slab(a, k):
        return remote(
            uown.at[a, pl.ds(share, slab)], ssf.at[pl.ds(pl.multiple_of(d * slab, 8), slab)],
            ss.at[k - 1], sr.at[k - 1], {"dp": lax.rem(d + k, nd)},
        )

    def slab_end(a):
        for k in range(1, nd):
            gather_slab(a, k).wait_recv()
        return ssf[...]

    def hop(a, k, owner, send, recv, to):
        at = u.at[a, place(owner, behind(k))]
        source = uown.at[a, pl.ds(0, share)] if k == 0 and send is not ks else at
        return remote(source, at, send.at[a, k], recv.at[a, k], {"mp": to})

    def to_facing(a, k):
        return hop(a, k, m, ys, yr, facing)

    def to_mate(a, k):
        return hop(a, k, m, cs, cr, mate)

    def on_to_mate(a, k):
        return hop(a, k, facing, ks, kr, mate)

    def sum_start(a, value, extra=None):
        some = exact_left(xb[pl.ds(pl.multiple_of(m * quarter, 8), quarter), :], value)
        upart[a, :, :share] = some.reshape(nd, share, rank)
        if extra is not None:
            upart[a, :, share:] = extra.reshape(nd, slab, rank)
        for k in range(1, nd):
            reduce(a, k).start()

    def sum_own(a):
        size = share + slab if a == 0 else share
        total = upart[a, d, :size]
        for k in range(1, nd):
            reduce(a, k).wait_recv()
            total = total + uland[a, behind(k), :size]
        uown[a, :size] = total
        if a == 0:
            for k in range(1, nd):
                gather_slab(a, k).start()
            ssf[pl.ds(pl.multiple_of(d * slab, 8), slab)] = total[share:]
        for k in range(1, nd):
            gather(a, k).start()
        to_facing(a, 0).start()
        to_mate(a, 0).start()
        u[a, place(m, d)] = total[:share]

    def sum_pass(a, ks_):
        for k in ks_:
            gather(a, k).wait_recv()
            to_facing(a, k).start()
            to_mate(a, k).start()

    def sum_cross(a, ks_):
        for k in ks_:
            hop(a, k, facing, ys, yr, facing).wait_recv()
            on_to_mate(a, k).start()

    def sum_end(a):
        for k in range(nd):
            to_mate(a, k).wait_recv()
            on_to_mate(a, k).wait_recv()

    def sum_drain(a):
        for k in range(1, nd):
            reduce(a, k).wait_send()
            gather(a, k).wait_send()
            if a == 0:
                gather_slab(a, k).wait_send()
        for k in range(nd):
            to_facing(a, k).wait_send()
            to_mate(a, k).wait_send()
            on_to_mate(a, k).wait_send()

    band = wland.shape[1]

    def band_of(owner):
        return pl.ds(pl.multiple_of(owner * band, 8), band)

    def part_out(k):
        return remote(wpart.at[band_of(m)], wland.at[d], vs.at[k - 1], vr.at[k - 1], {"dp": lax.rem(d + k, nd)})

    def part_share(n, owner, to):
        at = wsum.at[band_of(owner)]
        return remote(at, at, hs.at[n], hr.at[n], {"mp": to})

    def small_start(value):
        wpart[...] = value
        for k in range(1, nd):
            part_out(k).start()
        wland[d] = wpart[band_of(m)]

    def small_sum():
        for k in range(1, nd):
            part_out(k).wait_recv()
        total = wland[0]
        for n in range(1, nd):
            total = total + wland[n]
        wsum[band_of(m)] = total
        part_share(0, m, facing).start()
        part_share(1, m, mate).start()

    def small_pass():
        part_share(0, facing, facing).wait_recv()
        part_share(2, facing, mate).start()

    def small_end():
        part_share(1, m, mate).wait_recv()
        part_share(2, m, mate).wait_recv()
        return wsum[...]

    def small_drain():
        for k in range(1, nd):
            part_out(k).wait_send()
        for n in range(3):
            part_share(n, m, mate).wait_send()

    bands, half = w.shape[1], w.shape[3]

    def to_core(a, q):
        return remote(ppart.at[a, q, 1 - mc], pland.at[a, q], ps.at[a, q], pr.at[a, q], {"mp": mate})

    def to_chip(a, q):
        return remote(psum.at[a, q], pother.at[a, q], qs.at[a, q], qr.at[a, q], {"mp": facing})

    def back(a, q):
        at = w.at[a, q, mc]
        return remote(at, at, ts.at[a, q], tr.at[a, q], {"mp": mate})

    def images(a, value):
        span = exact_right(value.T, yb[...]).T
        both = halves(span, 1)
        for q in range(bands):
            some = jnp.dot(yb[q * 2 * half : (q + 1) * 2 * half, :], both, preferred_element_type=jnp.float32)
            ppart[a, q] = (folded(some, 1) * (scale * scale)).reshape(2, half, rank)
            to_core(a, q).start()

    def image_chip(a, q):
        to_core(a, q).wait_recv()
        psum[a, q] = ppart[a, q, mc] + pland[a, q]
        to_chip(a, q).start()

    def image_sum(a, q):
        to_chip(a, q).wait_recv()
        w[a, q, mc] = psum[a, q] + pother[a, q]
        back(a, q).start()

    def image_end(a):
        for q in range(bands):
            back(a, q).wait_recv()
        return w[a].reshape(count, rank)

    def image_drain(a):
        for q in range(bands):
            to_core(a, q).wait_send()
            to_chip(a, q).wait_send()
            back(a, q).wait_send()

    def first_sum():
        keep_x.wait()
        for k in range(1, nd):
            share_of(k, m, 1, mate).wait_recv()
            share_of(k, m, 2, mate).wait_recv()
        for s in range(nd):
            xt[:, s * rows : (s + 1) * rows] = xland[s].T.astype(jnp.bfloat16)
            xb[s * rows : (s + 1) * rows, :] = xland[s].astype(jnp.bfloat16)
        sketch = s_ref[...]
        sum_start(0, sketch, gram(sketch, sketch))

    def twin(way):
        at = yland.at[other, cuts[0]]
        n = (way + 1) // 2
        return remote(at, at, twins.at[n], twinr.at[n], {"dp": 2 * (z + way) + x})

    def by_twin(k, c):
        return k == 0 and c == 0

    def start_twins():
        over[0].wait_recv()
        for way in (1, -1):
            pl.when(inside(z + way))(lambda way=way: twin(way).start())

    def relay(steps):
        for way, k, c in steps:

            @pl.when(inside(z - way * (k + 1)))
            def _():
                along(way, k, c).wait_recv()
                if not by_twin(k, c):
                    across(way, k, c).start()

                if k + 1 < nz - 1:

                    @pl.when(inside(z + way))
                    def _():
                        along(way, k + 1, c).start()

    waves = streams(nz - 1)
    plan = {
        (0, 0): pass_on,
        (0, 1): first_sum,
        (1, 2): lambda: sum_own(0),
        (2, 2): lambda: sum_pass(0, range(1, nd)),
        (2, 3): lambda: sum_cross(0, range(nd)),
    }
    start_twins()
    for k in range(nz - 1):
        for c in range(pieces):
            relay([(way, k, c) for way in (1, -1)])
            plan.get((k, c), lambda: None)()
    sum_end(0)
    sketch_gram = slab_end(0)
    mixed0 = DECAY_RATE * times(u[0], sketch_gram)
    square_gram = DECAY_RATE * times(sketch_gram, sketch_gram)
    keep_y.wait()
    for copy in over[1:]:
        copy.wait_recv()
    for way, k, c in waves:
        last = twin(way).wait_recv if by_twin(k, c) else across(way, k, c).wait
        pl.when(inside(z - way * (k + 1)))(lambda last=last: last())
    for s in range(nd):
        yb[s * rows : (s + 1) * rows, :] = yland[s].astype(jnp.bfloat16)

    square = (rank, rank)
    diagonal = lax.broadcasted_iota(jnp.int32, square, 0) == lax.broadcasted_iota(jnp.int32, square, 1)
    tile = 256 if width % 256 == 0 else width

    def gradient_tile(t, carry):
        cols = pl.ds(pl.multiple_of(t * tile, 128), tile)
        g[:, cols] = scale * jnp.dot(xt[...], yb[:, cols], preferred_element_type=jnp.float32)
        return carry

    images(0, u[0])
    for q in range(bands):
        image_chip(0, q)
    lax.fori_loop(0, width // tile, gradient_tile, 0)
    for q in range(bands):
        image_sum(0, q)
    w0 = image_end(0)
    sum_start(1, exact_left(xt[...], w0))
    proj1 = square_gram + gram(u[0], w0)
    sum_own(1)
    sum_pass(1, range(1, nd))
    sum_cross(1, range(nd))
    sum_end(1)
    kept[...] = mixed0 + u[1]
    images(1, kept[...])
    gram_mat = DECAY_RATE * times(sketch_gram, proj1) + gram(w0, kept[...])
    low = []
    run_with(
        factor_steps(gram_mat, low),
        [lambda: None] * 3
        + [functools.partial(image_chip, 1, q) for q in range(bands)]
        + [lambda: None] * 4
        + [functools.partial(image_sum, 1, q) for q in range(bands)],
    )
    low_t = low[0].T
    w1 = times(image_end(1), low_t)
    moved = exact_left(xt[...], w1)
    proj1 = times(proj1, low_t)
    applied = DECAY_RATE * times(s_ref[...], proj1) + moved
    small_start(gram(applied, applied))
    sum_start(2, moved)
    u1 = times(kept[...], low_t)
    rayleigh = DECAY_RATE * gram(proj1, proj1) + gram(u1, w1)
    rayleigh = 0.5 * (rayleigh + rayleigh.T)
    mean_level = jnp.sum(jnp.where(diagonal, rayleigh, 0.0)) / rank
    shifted = rayleigh + jnp.where(diagonal, RIDGE_FRAC * mean_level, 0.0)
    top = []
    run_with(
        factor_steps(shifted, top),
        [lambda: None] * 9 + [small_sum, lambda: sum_own(2), lambda: None, lambda: None, lambda: None, small_pass],
    )
    inner = small_end() + mean_level * shifted
    bottom = []
    run_with(
        factor_steps(inner, bottom),
        [lambda: None] * 5
        + [functools.partial(sum_pass, 2, range(1, 4)), functools.partial(sum_pass, 2, range(4, nd))]
        + [lambda: None] * 2
        + [functools.partial(sum_cross, 2, range(4)), functools.partial(sum_cross, 2, range(4, nd))],
    )
    new_ref[...] = times(applied, top[0].T)
    mixed1 = DECAY_RATE * times(u[0], proj1)
    mixer = halves(times(times(applied, bottom[0].T), bottom[0]), 1)
    sum_end(2)
    u2 = mixed1 + u[2]
    span = scale * exact_right(u2.T, yb[...])
    span_ref[...] = span
    mixer_ref[...] = mixer

    for copy in pending:
        copy.wait_send()
    for way, k, c in waves:
        pl.when(sends(way, k))(lambda way=way, k=k, c=c: along(way, k, c).wait_send())
    for way in (1, -1):
        pl.when(inside(z + way))(lambda way=way: twin(way).wait_send())
    for a in range(3):
        sum_drain(a)
    for a in range(2):
        image_drain(a)
    small_drain()


def last_kernel(g_ref, mixer_ref, span_ref, new_in_ref, pre_ref, new_ref):
    new_ref[...] = new_in_ref[...]
    rank, width = span_ref.shape
    mixer = mixer_ref[...]
    tile = 256 if width % 256 == 0 else width
    for t in range(width // tile):
        cols = slice(t * tile, (t + 1) * tile)
        both = halves(span_ref[:, cols], 0)
        high = jnp.concatenate([both[:rank], both[:rank]], axis=0)
        low = jnp.concatenate([both[rank:], both[rank:]], axis=0)
        gone = jnp.dot(mixer, high, preferred_element_type=jnp.float32)
        gone = gone + jnp.dot(mixer, low, preferred_element_type=jnp.float32)
        pre_ref[:, cols] = (g_ref[:, cols] - gone).astype(jnp.bfloat16)


def last(gradient, mixer, span, new_sketch):
    return pl.pallas_call(
        last_kernel,
        out_shape=(
            jax.ShapeDtypeStruct(gradient.shape, jnp.bfloat16),
            jax.ShapeDtypeStruct(new_sketch.shape, jnp.float32),
        ),
        in_specs=[pl.BlockSpec(memory_space=VMEM)] * 4,
        out_specs=(pl.BlockSpec(memory_space=VMEM),) * 2,
        name="last",
    )(gradient, mixer, span, new_sketch)


def whole_fits(tokens, cotangent, sketch):
    nd, nm = lax.axis_size("dp"), lax.axis_size("mp")
    rows, depth = tokens.shape
    width = cotangent.shape[1]
    block, rank = sketch.shape
    need = 6 * rows * (depth + width) + nd * rows * (8 * block + 6 * width) + 4 * block * width
    need += 54 * nd * rows * rank
    return (
        nm == 4
        and nd % 2 == 0
        and nd <= 16
        and rank == 128
        and rows % 128 == 0
        and nd >= 8
        and block % 128 == 0
        and width % 128 == 0
        and rank % (8 * nd) == 0
        and need <= VMEM_BUDGET
    )


def whole(tokens, cotangent, sketch, norm_scale):
    nd, nm = lax.axis_size("dp"), lax.axis_size("mp")
    rows, depth = tokens.shape
    width = cotangent.shape[1]
    block, rank = sketch.shape
    nz = nd // 2
    pieces = 4
    share, slab, band, count = rows // nm, rank // nd, rank // nm, nd * rows
    bands = 4
    half = count // (2 * bands)
    dma = pltpu.SemaphoreType.DMA
    f32 = jnp.float32
    return pl.pallas_call(
        functools.partial(whole_kernel, nd, nm, pieces, norm_scale),
        out_shape=(
            jax.ShapeDtypeStruct((block, width), f32),
            jax.ShapeDtypeStruct((block, 2 * rank), jnp.bfloat16),
            jax.ShapeDtypeStruct((rank, width), f32),
            jax.ShapeDtypeStruct((block, rank), f32),
        ),
        in_specs=[pl.BlockSpec(memory_space=pl.ANY)] * 3,
        out_specs=(pl.BlockSpec(memory_space=VMEM),) * 4,
        scratch_shapes=[
            pltpu.VMEM((rows, depth), jnp.bfloat16),
            pltpu.VMEM((rows, width), jnp.bfloat16),
            pltpu.VMEM((block, rank), f32),
            dma((3,)),
            pltpu.VMEM((rows, depth), f32),
            pltpu.VMEM((rows, width), f32),
            pltpu.VMEM((nd, rows, block), f32),
            pltpu.VMEM((nd, rows, width), f32),
            pltpu.VMEM((block, count), jnp.bfloat16),
            pltpu.VMEM((count, block), jnp.bfloat16),
            pltpu.VMEM((count, width), jnp.bfloat16),
            pltpu.VMEM((3, nd, share + slab, rank), f32),
            pltpu.VMEM((3, nd, share + slab, rank), f32),
            pltpu.VMEM((3, share + slab, rank), f32),
            pltpu.VMEM((3, count, rank), f32),
            pltpu.VMEM((count, rank), f32),
            pltpu.VMEM((rank, rank), f32),
            pltpu.VMEM((rank, rank), f32),
            pltpu.VMEM((nd, band, rank), f32),
            pltpu.VMEM((rank, rank), f32),
            pltpu.VMEM((2, bands, 2, half, rank), f32),
            pltpu.VMEM((2, bands, half, rank), f32),
            pltpu.VMEM((2, bands, half, rank), f32),
            pltpu.VMEM((2, bands, half, rank), f32),
            pltpu.VMEM((2, bands, 2, half, rank), f32),
            dma((2,)),
            dma((nd - 1,)),
            dma((nd - 1,)),
            dma((nd - 1, nm - 1)),
            dma((nd - 1, nm - 1)),
            dma((2, nz - 1, pieces)),
            dma((2, nz - 1, pieces)),
            dma((2, nz - 1, pieces)),
            dma((2, nz - 1, pieces)),
            dma((pieces,)),
            dma((pieces,)),
            dma((2,)),
            dma((2,)),
        ]
        + [dma((3, nd - 1))] * 4
        + [dma((nd - 1,))] * 2
        + [dma((nd - 1,))] * 2
        + [dma((3,))] * 2
        + [dma((3, nd))] * 6
        + [dma((2, bands))] * 6,
        compiler_params=pltpu.CompilerParams(
            collective_id=6, has_side_effects=True, vmem_limit_bytes=60 * 2**20
        ),
        name="whole",
    )(tokens, cotangent, sketch)


def shards(tokens, cotangent, sketch):
    norm_scale = 1.0 / math.sqrt(tokens.shape[0] * lax.axis_size("dp"))
    if whole_fits(tokens, cotangent, sketch):
        return last(*whole(tokens, cotangent, sketch, norm_scale))
    gradient = gradient_block(tokens, cotangent, norm_scale)

    grad_proj, sketch_proj = all_sum(
        (product(gradient, sketch, TN), product(sketch, sketch, TN)), "dp", 1
    )
    (summed,) = all_sum((product(gradient, grad_proj),), "mp", 2)
    previous = DECAY_RATE * product(sketch, sketch_proj) + summed
    grad_image, sketch_image, gram_mat = all_sum(
        (
            product(gradient, previous, TN),
            product(sketch, previous, TN),
            product(previous, previous, TN),
        ),
        "dp",
        3,
    )
    summed, low_inv = all_sum((product(gradient, grad_image),), "mp", 4, gram_mat)
    applied = product(DECAY_RATE * product(sketch, sketch_image) + summed, low_inv, NT)
    image_grad, cross_prev, self_image = all_sum(
        (
            product(gradient, applied, TN),
            product(previous, applied, TN),
            product(applied, applied, TN),
        ),
        "dp",
        5,
    )
    new_inv, mixer = small_call(finish_kernel, 2, "finish", low_inv, cross_prev, self_image)
    new_sketch = product(applied, new_inv, NT)
    precond = gradient - product(product(new_sketch, mixer), image_grad, NT)
    return (precond.astype(jnp.bfloat16), new_sketch)


def solution(mesh):
    in_specs = (P("dp", None), P("dp", "mp"), P("dp", None))
    out_specs = (P("dp", "mp"), P("dp", None))
    return jax.shard_map(shards, mesh=mesh, in_specs=in_specs, out_specs=out_specs, check_vma=False)
```
